16 devices in a mesh: frag: 2 (over z), dev: 8 (over y, x, core).
Axes of the slice: x: 2, y: 2, z: 2, core: 2. Of those that a mesh axis runs over, the one named last changes fastest.
Arguments:
- a_ints: bfloat16 [208, 104, 104, 104], P(('frag', 'dev')), parts along dimension 0
- c_occ: bfloat16 [208, 32], P('frag'), parts along dimension 0
- c_vir: bfloat16 [208, 64], P('frag'), parts along dimension 0
- eps_occ: float32 [64], P('frag'), parts along dimension 0
- eps_vir: float32 [128], P('frag'), parts along dimension 0
Outputs:
- output: float32 [64, 32], P('frag', 'dev'), parts along dimension 0
There are 2 independent parts. The reference program is written for one: setup_inputs(seed, part) draws one part's arguments, and reference() takes and returns one part's arrays. A program takes and returns all parts, laid end to end along the dimension named above; each array names one.
All inputs are finite; a program needn't handle non-finite values.
Results may differ from the reference program's by a relative error of at most 0.001.
Values are sent between devices in bfloat16 or wider.
A program may use at most 1 GiB of HBM per device.

```python
import jax
import jax.numpy as jnp
from jax import lax

PAD_BASIS = 104
NUM_OCC = 32
NUM_VIRT = 64


def setup_inputs(seed: int = 0, part: int = 0) -> dict:
    key_base = jax.random.fold_in(jax.random.key(seed), part)
    key_ints, key_occ, key_vir, key_eocc, key_evir = jax.random.split(key_base, 5)

    def draw_row(row_idx):
        raw_row = jax.random.normal(jax.random.fold_in(key_ints, row_idx), (PAD_BASIS, PAD_BASIS, PAD_BASIS), jnp.float32)
        mixed_row = (raw_row + 0.5 * jnp.transpose(raw_row, (2, 1, 0))) * (1.25 ** -0.5)
        return mixed_row.astype(jnp.bfloat16)

    a_ints = lax.map(draw_row, jnp.arange(PAD_BASIS))
    c_occ = (jax.random.normal(key_occ, (PAD_BASIS, NUM_OCC), jnp.float32) * PAD_BASIS ** -0.5).astype(jnp.bfloat16)
    c_vir = (jax.random.normal(key_vir, (PAD_BASIS, NUM_VIRT), jnp.float32) * (PAD_BASIS * NUM_VIRT) ** -0.5).astype(jnp.bfloat16)
    eps_occ = jax.random.uniform(key_eocc, (NUM_OCC,), jnp.float32, -1.5, -0.5)
    eps_vir = jax.random.uniform(key_evir, (NUM_VIRT,), jnp.float32, 0.3, 2.0)
    return {"a_ints": a_ints, "c_occ": c_occ, "c_vir": c_vir, "eps_occ": eps_occ, "eps_vir": eps_vir}


def reference(a_ints, c_occ, c_vir, eps_occ, eps_vir):
    occ_32 = c_occ.astype(jnp.float32)
    vir_32 = c_vir.astype(jnp.float32)

    def first_half(a_row):
        t_one = jnp.einsum("qrs,rj->qsj", a_row.astype(jnp.float32), occ_32).astype(jnp.bfloat16)
        return jnp.einsum("qsj,sb->qjb", t_one.astype(jnp.float32), vir_32).astype(jnp.bfloat16)

    half_mo = lax.map(first_half, a_ints)
    g_mat = jnp.einsum("pqjb,qa->pjba", half_mo.astype(jnp.float32), vir_32).astype(jnp.bfloat16)
    v_mo = jnp.einsum("pjba,pi->jbai", g_mat.astype(jnp.float32), occ_32)
    v_swap = jnp.swapaxes(v_mo, 1, 2)
    denominator = (eps_occ[:, None, None, None] + eps_occ[None, None, None, :]
                   - eps_vir[None, :, None, None] - eps_vir[None, None, :, None])
    pair_ji = jnp.sum(v_mo * (2.0 * v_mo - v_swap) / denominator, axis=(1, 2))
    return pair_ji.T
```

```python
import functools

import jax
import jax.numpy as jnp
from jax import lax
from jax.experimental import pallas as pl
from jax.experimental.pallas import tpu as pltpu
from jax.sharding import PartitionSpec as P


MESH = pl.DeviceIdType.MESH
SUB = 16
F32 = jnp.float32
BF16 = jnp.bfloat16


def iota(shape, dim):
    return lax.broadcasted_iota(jnp.int32, shape, dim)


def ones_where(cond):
    return jnp.where(cond, 1.0, 0.0).astype(BF16)


def dot(a, b):
    return jnp.dot(a, b, preferred_element_type=F32)


def dot_t(a, b):
    return lax.dot_general(a, b, (((1,), (1,)), ((), ())), preferred_element_type=F32)


def kernel(n, o, v, group, rows, a_hbm, cot_ref, cvt_ref, eo_ref, ev_ref, e_ref,
           abuf, l1, w2, l3, l4, tp, hs, gsend, recv, vacc, rden, esum, a_sem, send_sem, recv_sem):
    me = lax.axis_index("dev")
    slots = abuf.shape[0]
    block = 2 * v

    def load(p, slot):
        return pltpu.make_async_copy(a_hbm.at[p], abuf.at[slot], a_sem.at[slot])

    for p in range(slots):
        load(p, p).start()

    def peer(k):
        core, x, y = lax.rem(me, 2), lax.rem(me // 2, 2), me // 4
        return 4 * lax.rem(y + k // 4, 2) + 2 * lax.rem(x + k // 2 % 2, 2) + lax.rem(core + k % 2, 2)

    barrier = pltpu.get_barrier_semaphore()
    for k in range(1, group):
        pl.semaphore_signal(barrier, inc=1, device_id={"dev": peer(k)}, device_id_type=MESH)

    row = iota((64, o), 0)
    perm = ones_where(2 * (row % SUB) + row // SUB % 2 == iota((64, o), 1))
    cotp = dot(perm, cot_ref[...]).astype(BF16)
    spread = ones_where(iota((n, 2 * n), 1) % n == iota((n, 2 * n), 0))
    same = iota((64, 2 * n), 0) // 32 == iota((64, 2 * n), 1) // n
    l1[...] = jnp.where(same, dot(cotp, spread), 0.0).astype(BF16)
    spread = ones_where(iota((256, n), 0) % 128 == iota((256, n), 1))
    same = iota((256, 2 * v), 0) // 128 == iota((256, 2 * v), 1) // v
    cvt2 = jnp.concatenate([cvt_ref[...], cvt_ref[...]], axis=0)
    w2[...] = jnp.where(same, dot_t(spread, cvt2), 0.0).astype(BF16)
    spread = ones_where(iota((n, SUB * n), 1) // SUB == iota((n, SUB * n), 0))
    cvrep = dot(cvt_ref[...], spread)
    for j in range(SUB):
        l3[j * v:(j + 1) * v, :] = jnp.where(iota((v, SUB * n), 1) % SUB == j, cvrep, 0.0).astype(BF16)

    def send(p, k):
        return pltpu.make_async_remote_copy(
            src_ref=gsend.at[p, pl.ds(pl.multiple_of(peer(k) * block, block), block)],
            dst_ref=recv.at[p, me],
            send_sem=send_sem,
            recv_sem=recv_sem.at[p],
            device_id={"dev": peer(k)},
            device_id_type=MESH,
        )

    pad = jnp.zeros((2 * n, 128 - n), BF16)

    def make_g(p):
        slot = lax.rem(p, slots)
        load(p, slot).wait()

        def tile(t, carry):
            base = pl.multiple_of(t * 4 * n, SUB)
            left = abuf[slot, pl.ds(base, 2 * n), :]
            right = abuf[slot, pl.ds(base + 2 * n, 2 * n), :]
            out = dot(l1[...], jnp.concatenate([left, pad, right, pad], axis=1)).astype(BF16)
            for qn in range(2):
                for qk in range(2):
                    to = pl.ds(pl.multiple_of(t * 64 + (2 * qn + qk) * SUB, SUB), SUB)
                    for jh in range(2):
                        at = qk * 32 + jh * SUB
                        tp[to, jh * 128:(jh + 1) * 128] = out[at:at + SUB, qn * 128:(qn + 1) * 128]
            return carry

        lax.fori_loop(0, n // 4, tile, 0, unroll=n // 4)
        hs[...] = dot(tp[...], w2[...]).astype(BF16)
        gsend[p] = dot(l3[...], hs[...]).astype(BF16)

        @pl.when(p + slots < rows)
        def _():
            load(p + slots, slot).start()

    make_g(0)
    pl.semaphore_wait(barrier, group - 1)

    def hand_out(p):
        for k in (6, 7, 4, 5, 2, 3, 1):
            send(p, k).start()
        recv[p, me] = gsend[p, pl.ds(pl.multiple_of(me * block, block), block), :]

    hand_out(0)

    @pl.loop(1, rows)
    def _(p):
        make_g(p)
        hand_out(p)

    lane = iota((n, SUB * n), 1) // SUB
    spread = ones_where(lane % group * rows + lane // group == iota((n, SUB * n), 0))
    corep = dot(cot_ref[...], spread).astype(BF16)
    split = ones_where(iota((SUB * o, o), 0) // SUB == iota((SUB * o, o), 1))
    diag = iota((SUB * o, SUB * n), 0) % SUB == iota((SUB * o, SUB * n), 1) % SUB
    l4[...] = jnp.where(diag, dot(split, corep), 0.0).astype(BF16)

    ev = ev_ref[...]
    ev_b = jnp.concatenate([ev, ev], axis=1)
    ev_a = jnp.transpose(jnp.broadcast_to(ev_b, (128, 128)))
    at = me * (o // group)
    first = iota((128, 128), 0) < v
    even = iota((128, 128), 1) < v
    eo_j = jnp.where(first, jnp.where(even, eo_ref[at], eo_ref[at + 1]),
                     jnp.where(even, eo_ref[at + 2], eo_ref[at + 3]))

    @pl.loop(0, o)
    def _(i):
        rden[i] = 1.0 / (eo_j + eo_ref[i] - ev_a - ev_b)

    def arrived(p):
        pltpu.make_async_remote_copy(
            src_ref=recv.at[p, pl.ds(0, group - 1)],
            dst_ref=recv.at[p, pl.ds(0, group - 1)],
            send_sem=send_sem,
            recv_sem=recv_sem.at[p],
            device_id={"dev": peer(1)},
            device_id_type=MESH,
        ).wait_recv()

    def add(lo, hi):
        for p in range(lo, hi):
            arrived(p)
        depth = (hi - lo) * group * SUB
        for g in range(v // SUB):
            parts = [recv[lo:hi, :, x * v + g * SUB:x * v + (g + 1) * SUB, :].reshape(depth, 128) for x in range(2)]
            part = dot(l4[:, lo * group * SUB:hi * group * SUB], jnp.concatenate(parts, axis=1))
            vacc[g] = part if lo == 0 else vacc[g] + part

    add(0, 8)
    add(8, 12)
    add(12, rows)

    @pl.loop(0, o, unroll=4)
    def _(i):
        at = pl.ds(pl.multiple_of(i * SUB, SUB), SUB)
        halves = [jnp.concatenate([vacc[g, at, x * 128:(x + 1) * 128] for g in range(v // SUB)], axis=0)
                  for x in range(2)]
        mat = jnp.concatenate(halves, axis=0)
        mat_t = jnp.transpose(mat)
        turned = pltpu.roll(jnp.concatenate([mat_t[v:], mat_t[:v]], axis=0), v, 1)
        swap = jnp.where(first == even, mat_t, turned)
        term = mat * (2.0 * mat - swap) * rden[i]
        for x in range(2):
            esum[x, i] = jnp.sum(term[x * v:(x + 1) * v].reshape(v // 8, 8, 128), axis=0)

    lane = iota((o, 128), 1)
    out = jnp.zeros((o, 128), F32)
    for x in range(2):
        both = jnp.sum(esum[x], axis=1)
        for jh in range(2):
            total = jnp.sum(jnp.where(lane // v == jh, both, 0.0), axis=1, keepdims=True)
            out = jnp.where(lane == 2 * x + jh, total, out)
    e_ref[...] = out[:, :o // group]

    pltpu.make_async_remote_copy(
        src_ref=gsend.at[:, pl.ds(0, (group - 1) * block)],
        dst_ref=gsend.at[:, pl.ds(0, (group - 1) * block)],
        send_sem=send_sem,
        recv_sem=recv_sem.at[0],
        device_id={"dev": peer(1)},
        device_id_type=MESH,
    ).wait_send()


def solution(mesh):
    group = mesh.shape["dev"]

    def per_device(a_ints, c_occ, c_vir, eps_occ, eps_vir):
        rows, n = a_ints.shape[:2]
        o, v = c_occ.shape[1], c_vir.shape[1]
        vmem = pl.BlockSpec(memory_space=pltpu.VMEM)
        return pl.pallas_call(
            functools.partial(kernel, n, o, v, group, rows),
            out_shape=jax.ShapeDtypeStruct((o, o // group), F32),
            in_specs=[pl.BlockSpec(memory_space=pl.ANY), vmem, vmem,
                      pl.BlockSpec(memory_space=pltpu.SMEM), vmem],
            out_specs=vmem,
            scratch_shapes=[
                pltpu.VMEM((3, n * n, n), BF16),
                pltpu.VMEM((64, 2 * n), BF16),
                pltpu.VMEM((256, 128), BF16),
                pltpu.VMEM((SUB * v, SUB * n), BF16),
                pltpu.VMEM((SUB * o, SUB * n), BF16),
                pltpu.VMEM((SUB * n, 256), BF16),
                pltpu.VMEM((SUB * n, 128), BF16),
                pltpu.VMEM((rows, SUB * v, 128), BF16),
                pltpu.VMEM((rows, group, 2 * v, 128), BF16),
                pltpu.VMEM((v // SUB, SUB * o, 256), F32),
                pltpu.VMEM((o, 128, 128), F32),
                pltpu.VMEM((2, o, 8, 128), F32),
                pltpu.SemaphoreType.DMA((3,)),
                pltpu.SemaphoreType.DMA,
                pltpu.SemaphoreType.DMA((rows,)),
            ],
            compiler_params=pltpu.CompilerParams(
                collective_id=0, has_side_effects=True, vmem_limit_bytes=60 * 2**20),
        )(a_ints.reshape(rows, n * n, n), c_occ.T, c_vir.T, eps_occ, eps_vir.reshape(1, v))

    return jax.shard_map(
        per_device,
        mesh=mesh,
        in_specs=(P(("frag", "dev")), P("frag"), P("frag"), P("frag"), P("frag")),
        out_specs=P("frag", "dev"),
        check_vma=False,
    )
```

```python
import functools

import jax
import jax.numpy as jnp
from jax import lax
from jax.experimental import pallas as pl
from jax.experimental.pallas import tpu as pltpu
from jax.sharding import PartitionSpec as P


MESH = pl.DeviceIdType.MESH
SUB = 16
LATE = 5
FAR, NEAR = (6, 7, 4, 5), (2, 3, 1)
F32 = jnp.float32
BF16 = jnp.bfloat16


def iota(shape, dim):
    return lax.broadcasted_iota(jnp.int32, shape, dim)


def ones_where(cond):
    return jnp.where(cond, 1.0, 0.0).astype(BF16)


def dot(a, b):
    return jnp.dot(a, b, preferred_element_type=F32)


def dot_t(a, b):
    return lax.dot_general(a, b, (((1,), (1,)), ((), ())), preferred_element_type=F32)


def kernel(n, o, v, group, rows, a_hbm, cot_hbm, cvt_hbm, eo_hbm, ev_hbm, e_ref,
           abuf, cot, cvt, eo, ev_ref, l1, w2, l3, l4, tp, hs, gsend, recv, vacc, rden, esum,
           a_sem, in_sem, send_sem, recv_sem):
    me = lax.axis_index("dev")
    slots = abuf.shape[0]
    tiles = n // 4
    cuts = [tiles * c // 26 for c in (0, 9, 17, 23, 26)]

    def load(p, slot):
        return pltpu.make_async_copy(a_hbm.at[p], abuf.at[slot], a_sem.at[slot])

    def load_first(c):
        at = pl.ds(cuts[c] * 4 * n, (cuts[c + 1] - cuts[c]) * 4 * n)
        return pltpu.make_async_copy(a_hbm.at[0, at], abuf.at[0, at], in_sem.at[4 + c])

    small = [pltpu.make_async_copy(src, dst, in_sem.at[k]) for k, (src, dst) in enumerate(
        [(cot_hbm, cot), (cvt_hbm, cvt), (eo_hbm, eo), (ev_hbm, ev_ref)])]
    for copy in small:
        copy.start()
    for c in range(4):
        load_first(c).start()

    def peer(k):
        core, x, y = lax.rem(me, 2), lax.rem(me // 2, 2), me // 4
        return 4 * lax.rem(y + k // 4, 2) + 2 * lax.rem(x + k // 2 % 2, 2) + lax.rem(core + k % 2, 2)

    barrier = pltpu.get_barrier_semaphore()
    for k in range(1, group):
        pl.semaphore_signal(barrier, inc=1, device_id={"dev": peer(k)}, device_id_type=MESH)
    for copy in small:
        copy.wait()

    row = iota((64, o), 0)
    perm = ones_where(2 * (row % SUB) + row // SUB % 2 == iota((64, o), 1))
    cotp = dot(perm, cot[...]).astype(BF16)
    spread = ones_where(iota((n, 2 * n), 1) % n == iota((n, 2 * n), 0))
    same = iota((64, 2 * n), 0) // 32 == iota((64, 2 * n), 1) // n
    l1[...] = jnp.where(same, dot(cotp, spread), 0.0).astype(BF16)
    spread = ones_where(iota((256, n), 0) % 128 == iota((256, n), 1))
    same = iota((256, 2 * v), 0) // 128 == iota((256, 2 * v), 1) // v
    cvt2 = jnp.concatenate([cvt[...], cvt[...]], axis=0)
    w2[...] = jnp.where(same, dot_t(spread, cvt2), 0.0).astype(BF16)
    spread = ones_where(iota((n, SUB * n), 1) // SUB == iota((n, SUB * n), 0))
    cvrep = dot(cvt[...], spread).astype(BF16)
    for j in range(SUB):
        pick = (iota((v, SUB * n), 1) % SUB == j)
        l3[j * v:(j + 1) * v, :] = jnp.where(pick, cvrep, jnp.zeros_like(cvrep))

    def send(p, x, k):
        return pltpu.make_async_remote_copy(
            src_ref=gsend.at[p, pl.ds(pl.multiple_of((2 * peer(k) + x) * v, v), v)],
            dst_ref=recv.at[x, p, me],
            send_sem=send_sem,
            recv_sem=recv_sem.at[x, p],
            device_id={"dev": peer(k)},
            device_id_type=MESH,
        )

    pad = jnp.zeros((2 * n, 128 - n), BF16)

    def tile(slot, t):
        base = t * 4 * n if isinstance(t, int) else pl.multiple_of(t * 4 * n, SUB)
        left = abuf[slot, pl.ds(base, 2 * n), :]
        right = abuf[slot, pl.ds(base + 2 * n, 2 * n), :]
        out = dot(l1[...], jnp.concatenate([left, pad, right, pad], axis=1)).astype(BF16)
        for qn in range(2):
            for qk in range(2):
                to = t * 64 + (2 * qn + qk) * SUB
                to = pl.ds(to if isinstance(t, int) else pl.multiple_of(to, SUB), SUB)
                for jh in range(2):
                    at = qk * 32 + jh * SUB
                    tp[to, jh * 128:(jh + 1) * 128] = out[at:at + SUB, qn * 128:(qn + 1) * 128]

    def finish(p, chip, chips):
        at = pl.ds(pl.multiple_of(chip * 4 * v, 4 * v), chips * 4 * v)
        gsend[p, at, :] = dot(l3[at, :], hs[...]).astype(BF16)

    def hand_out(p, ks, xs):
        for x in xs:
            for k in ks:
                send(p, x, k).start()

    def keep(p):
        for x in range(2):
            recv[x, p, me] = gsend[p, pl.ds(pl.multiple_of((2 * me + x) * v, v), v), :]

    for c in range(4):
        load_first(c).wait()
        if c == 2:
            for p in range(1, slots):
                load(p, p).start()
        for t in range(cuts[c], cuts[c + 1]):
            tile(0, t)
        at = slice(cuts[c] * 64, cuts[c + 1] * 64)
        hs[at, :] = dot(tp[at, :], w2[...]).astype(BF16)
    load(slots, 0).start()
    finish(0, peer(6) // 2, 1)
    pl.semaphore_wait(barrier, group - 1)
    hand_out(0, (6, 7), (0, 1))
    finish(0, peer(4) // 2, 1)
    hand_out(0, (4, 5), (0, 1))
    finish(0, me // 4 * 2, 2)
    hand_out(0, NEAR, (0, 1))
    keep(0)

    @pl.loop(1, rows)
    def _(p):
        slot = lax.rem(p, slots)
        load(p, slot).wait()
        lax.fori_loop(0, tiles, lambda t, _: tile(slot, t), None, unroll=tiles)

        @pl.when(p + slots < rows)
        def _():
            load(p + slots, slot).start()

        hs[...] = dot(tp[...], w2[...]).astype(BF16)
        gsend[p] = dot(l3[...], hs[...]).astype(BF16)
        hand_out(p, FAR + NEAR, (0,))

        @pl.when(p < rows - LATE)
        def _():
            hand_out(p, FAR + NEAR, (1,))

        keep(p)

    @pl.loop(rows - LATE, rows)
    def _(p):
        hand_out(p, FAR + NEAR, (1,))

    lane = iota((n, SUB * n), 1) // SUB
    spread = ones_where(lane % group * rows + lane // group == iota((n, SUB * n), 0))
    corep = dot(cot[...], spread).astype(BF16)
    split = ones_where(iota((SUB * o, o), 0) // SUB == iota((SUB * o, o), 1))
    diag = iota((SUB * o, SUB * n), 0) % SUB == iota((SUB * o, SUB * n), 1) % SUB
    l4[...] = jnp.where(diag, dot(split, corep), 0.0).astype(BF16)

    ev = ev_ref[...]
    ev_b = jnp.concatenate([ev, ev], axis=1)
    ev_a = jnp.transpose(jnp.broadcast_to(ev_b, (128, 128)))
    first = iota((128, 128), 0) < v
    even = iota((128, 128), 1) < v

    @pl.loop(0, o // 2)
    def _(i):
        eo_i = jnp.where(first, eo[2 * i], eo[2 * i + 1])
        for x in range(2):
            at = me * (o // group) + 2 * x
            eo_j = jnp.where(even, eo[at], eo[at + 1])
            rden[x, i] = 1.0 / (eo_i + eo_j - ev_a - ev_b)

    def arrived(x, p):
        pltpu.make_async_remote_copy(
            src_ref=recv.at[x, p, pl.ds(0, group - 1)],
            dst_ref=recv.at[x, p, pl.ds(0, group - 1)],
            send_sem=send_sem,
            recv_sem=recv_sem.at[x, p],
            device_id={"dev": peer(1)},
            device_id_type=MESH,
        ).wait_recv()

    def add(x, lo, hi):
        for p in range(lo, hi):
            arrived(x, p)
        depth = (hi - lo) * group * SUB
        for h in range(2):
            parts = [recv[x, lo:hi, :, (2 * h + g) * SUB:(2 * h + g + 1) * SUB, :].reshape(depth, 128) for g in range(2)]
            part = dot(l4[:, lo * group * SUB:hi * group * SUB], jnp.concatenate(parts, axis=1))
            vacc[x, h] = part if lo == 0 else vacc[x, h] + part

    def energies(x):
        @pl.loop(0, o // 2, unroll=o // 2)
        def _(i):
            mats = []
            for i2 in range(2):
                at = pl.ds(pl.multiple_of((2 * i + i2) * SUB, SUB), SUB)
                mats += [vacc[x, g // 2, at, g % 2 * 128:(g % 2 + 1) * 128] for g in range(v // SUB)]
            mat = jnp.concatenate(mats, axis=0)
            mat_t = jnp.transpose(mat)
            turned = pltpu.roll(jnp.concatenate([mat_t[v:], mat_t[:v]], axis=0), v, 1)
            swap = jnp.where(first == even, mat_t, turned)
            term = mat * (2.0 * mat - swap) * rden[x, i]
            for i2 in range(2):
                esum[x, 2 * i + i2] = jnp.sum(term[i2 * v:(i2 + 1) * v].reshape(v // 8, 8, 128), axis=0)

    lane = iota((o, 128), 1)
    out = jnp.zeros((o, 128), F32)
    for x in range(2):
        add(x, 0, 8)
        add(x, 8, 12)
        add(x, 12, rows)
        energies(x)
        both = jnp.sum(esum[x], axis=1)
        for jh in range(2):
            total = jnp.sum(jnp.where(lane // v == jh, both, 0.0), axis=1, keepdims=True)
            out = jnp.where(lane == 2 * x + jh, total, out)
    e_ref[...] = jnp.transpose(out)[:o // group, :]

    pltpu.make_async_remote_copy(
        src_ref=gsend.at[:, pl.ds(0, (group - 1) * 2 * v)],
        dst_ref=gsend.at[:, pl.ds(0, (group - 1) * 2 * v)],
        send_sem=send_sem,
        recv_sem=recv_sem.at[0, 0],
        device_id={"dev": peer(1)},
        device_id_type=MESH,
    ).wait_send()


def solution(mesh):
    group = mesh.shape["dev"]

    def per_device(a_ints, c_occ, c_vir, eps_occ, eps_vir):
        rows, n = a_ints.shape[:2]
        o, v = c_occ.shape[1], c_vir.shape[1]
        hbm = pl.BlockSpec(memory_space=pltpu.HBM)
        return pl.pallas_call(
            functools.partial(kernel, n, o, v, group, rows),
            out_shape=jax.ShapeDtypeStruct((o // group, o), F32),
            in_specs=[hbm] * 5,
            out_specs=pl.BlockSpec(memory_space=pltpu.VMEM),
            scratch_shapes=[
                pltpu.VMEM((3, n * n, n), BF16),
                pltpu.VMEM((o, n), BF16),
                pltpu.VMEM((v, n), BF16),
                pltpu.SMEM((o,), F32),
                pltpu.VMEM((1, v), F32),
                pltpu.VMEM((64, 2 * n), BF16),
                pltpu.VMEM((256, 128), BF16),
                pltpu.VMEM((SUB * v, SUB * n), BF16),
                pltpu.VMEM((SUB * o, SUB * n), BF16),
                pltpu.VMEM((SUB * n, 256), BF16),
                pltpu.VMEM((SUB * n, 128), BF16),
                pltpu.VMEM((rows, SUB * v, 128), BF16),
                pltpu.VMEM((2, rows, group, v, 128), BF16),
                pltpu.VMEM((2, 2, SUB * o, 256), F32),
                pltpu.VMEM((2, o // 2, 128, 128), F32),
                pltpu.VMEM((2, o, 8, 128), F32),
                pltpu.SemaphoreType.DMA((3,)),
                pltpu.SemaphoreType.DMA((8,)),
                pltpu.SemaphoreType.DMA,
                pltpu.SemaphoreType.DMA((2, rows)),
            ],
            compiler_params=pltpu.CompilerParams(
                collective_id=0, has_side_effects=True, vmem_limit_bytes=60 * 2**20),
        )(a_ints.reshape(rows, n * n, n), c_occ.T, c_vir.T, eps_occ, eps_vir.reshape(1, v)).T

    return jax.shard_map(
        per_device,
        mesh=mesh,
        in_specs=(P(("frag", "dev")), P("frag"), P("frag"), P("frag"), P("frag")),
        out_specs=P("frag", "dev"),
        check_vma=False,
    )
```

```python
import functools

import jax
import jax.numpy as jnp
from jax import lax
from jax.experimental import pallas as pl
from jax.experimental.pallas import tpu as pltpu
from jax.sharding import PartitionSpec as P


MESH = pl.DeviceIdType.MESH
SUB = 16
LATE = 5
FAR, NEAR = (6, 7, 4, 5), (2, 3, 1)
F32 = jnp.float32
BF16 = jnp.bfloat16


def iota(shape, dim):
    return lax.broadcasted_iota(jnp.int32, shape, dim)


def ones_where(cond):
    return jnp.where(cond, 1.0, 0.0).astype(BF16)


def dot(a, b):
    return jnp.dot(a, b, preferred_element_type=F32)


def dot_t(a, b):
    return lax.dot_general(a, b, (((1,), (1,)), ((), ())), preferred_element_type=F32)


def kernel(n, o, v, group, rows, a_hbm, cot_hbm, cvt_hbm, eo_hbm, ev_hbm, e_ref,
           abuf, cot, cvt, eo, ev_ref, l1, w2, l3, l4, tp, hs, gsend, recv, vacc, rden, esum,
           a_sem, in_sem, send_sem, recv_sem):
    me = lax.axis_index("dev")
    slots = abuf.shape[0]
    tiles = n // 4
    cuts = [tiles * c // 26 for c in (0, 9, 17, 23, 26)]

    def load(p, slot):
        return pltpu.make_async_copy(a_hbm.at[p], abuf.at[slot], a_sem.at[slot])

    def load_first(c):
        at = pl.ds(cuts[c] * 4 * n, (cuts[c + 1] - cuts[c]) * 4 * n)
        return pltpu.make_async_copy(a_hbm.at[0, at], abuf.at[0, at], in_sem.at[4 + c])

    small = [pltpu.make_async_copy(src, dst, in_sem.at[k]) for k, (src, dst) in enumerate(
        [(cot_hbm, cot), (cvt_hbm, cvt), (eo_hbm, eo), (ev_hbm, ev_ref)])]
    for copy in small:
        copy.start()
    for c in range(4):
        load_first(c).start()

    def peer(k):
        core, x, y = lax.rem(me, 2), lax.rem(me // 2, 2), me // 4
        return 4 * lax.rem(y + k // 4, 2) + 2 * lax.rem(x + k // 2 % 2, 2) + lax.rem(core + k % 2, 2)

    barrier = pltpu.get_barrier_semaphore()
    for k in range(1, group):
        pl.semaphore_signal(barrier, inc=1, device_id={"dev": peer(k)}, device_id_type=MESH)
    for copy in small:
        copy.wait()

    row = iota((64, o), 0)
    perm = ones_where(2 * (row % SUB) + row // SUB % 2 == iota((64, o), 1))
    cotp = dot(perm, cot[...]).astype(BF16)
    spread = ones_where(iota((n, 2 * n), 1) % n == iota((n, 2 * n), 0))
    same = iota((64, 2 * n), 0) // 32 == iota((64, 2 * n), 1) // n
    l1[...] = jnp.where(same, dot(cotp, spread), 0.0).astype(BF16)
    spread = ones_where(iota((256, n), 0) % 128 == iota((256, n), 1))
    same = iota((256, 2 * v), 0) // 128 == iota((256, 2 * v), 1) // v
    cvt2 = jnp.concatenate([cvt[...], cvt[...]], axis=0)
    w2[...] = jnp.where(same, dot_t(spread, cvt2), 0.0).astype(BF16)
    spread = ones_where(iota((n, SUB * n), 1) // SUB == iota((n, SUB * n), 0))
    cvrep = dot(cvt[...], spread).astype(BF16)
    for j in range(SUB):
        pick = (iota((v, SUB * n), 1) % SUB == j)
        l3[j * v:(j + 1) * v, :] = jnp.where(pick, cvrep, jnp.zeros_like(cvrep))

    def send(p, x, k):
        return pltpu.make_async_remote_copy(
            src_ref=gsend.at[p, pl.ds(pl.multiple_of((2 * peer(k) + x) * v, v), v)],
            dst_ref=recv.at[x, p, me],
            send_sem=send_sem,
            recv_sem=recv_sem.at[x, p],
            device_id={"dev": peer(k)},
            device_id_type=MESH,
        )

    pad = jnp.zeros((2 * n, 128 - n), BF16)

    def tile(slot, t):
        base = t * 4 * n if isinstance(t, int) else pl.multiple_of(t * 4 * n, SUB)
        left = abuf[slot, pl.ds(base, 2 * n), :]
        right = abuf[slot, pl.ds(base + 2 * n, 2 * n), :]
        out = dot(l1[...], jnp.concatenate([left, pad, right, pad], axis=1)).astype(BF16)
        for qn in range(2):
            for qk in range(2):
                to = t * 64 + (2 * qn + qk) * SUB
                to = pl.ds(to if isinstance(t, int) else pl.multiple_of(to, SUB), SUB)
                for jh in range(2):
                    at = qk * 32 + jh * SUB
                    tp[to, jh * 128:(jh + 1) * 128] = out[at:at + SUB, qn * 128:(qn + 1) * 128]

    def finish(p, chip, chips):
        at = pl.ds(pl.multiple_of(chip * 4 * v, 4 * v), chips * 4 * v)
        gsend[p, at, :] = dot(l3[at, :], hs[...]).astype(BF16)

    def hand_out(p, ks, xs):
        for x in xs:
            for k in ks:
                send(p, x, k).start()

    def keep(p):
        for x in range(2):
            recv[x, p, me] = gsend[p, pl.ds(pl.multiple_of((2 * me + x) * v, v), v), :]

    for c in range(4):
        load_first(c).wait()
        if c == 2:
            for p in range(1, slots):
                load(p, p).start()
        for t in range(cuts[c], cuts[c + 1]):
            tile(0, t)
        at = slice(cuts[c] * 64, cuts[c + 1] * 64)
        hs[at, :] = dot(tp[at, :], w2[...]).astype(BF16)
    load(slots, 0).start()
    finish(0, peer(6) // 2, 1)
    pl.semaphore_wait(barrier, group - 1)
    hand_out(0, (6, 7), (0, 1))
    finish(0, peer(4) // 2, 1)
    hand_out(0, (4, 5), (0, 1))
    finish(0, me // 4 * 2, 2)
    hand_out(0, NEAR, (0, 1))
    keep(0)

    @pl.loop(1, rows)
    def _(p):
        slot = lax.rem(p, slots)
        load(p, slot).wait()
        lax.fori_loop(0, tiles, lambda t, _: tile(slot, t), None, unroll=tiles)

        @pl.when(p + slots < rows)
        def _():
            load(p + slots, slot).start()

        hs[...] = dot(tp[...], w2[...]).astype(BF16)
        gsend[p] = dot(l3[...], hs[...]).astype(BF16)
        hand_out(p, FAR + NEAR, (0,))

        @pl.when(p < rows - LATE)
        def _():
            hand_out(p, FAR + NEAR, (1,))

        keep(p)

    @pl.loop(rows - LATE, rows)
    def _(p):
        hand_out(p, FAR + NEAR, (1,))

    lane = iota((n, SUB * n), 1) // SUB
    spread = ones_where(lane % group * rows + lane // group == iota((n, SUB * n), 0))
    corep = dot(cot[...], spread).astype(BF16)
    split = ones_where(iota((SUB * o, o), 0) // SUB == iota((SUB * o, o), 1))
    diag = iota((SUB * o, SUB * n), 0) % SUB == iota((SUB * o, SUB * n), 1) % SUB
    l4[...] = jnp.where(diag, dot(split, corep), 0.0).astype(BF16)

    ev = ev_ref[...]
    ev_b = jnp.concatenate([ev, ev], axis=1)
    ev_a = jnp.transpose(jnp.broadcast_to(ev_b, (128, 128)))
    first = iota((128, 128), 0) < v
    even = iota((128, 128), 1) < v

    @pl.loop(0, o // 2)
    def _(i):
        eo_i = jnp.where(first, eo[2 * i], eo[2 * i + 1])
        for x in range(2):
            at = me * (o // group) + 2 * x
            eo_j = jnp.where(even, eo[at], eo[at + 1])
            rden[x, i] = 1.0 / (eo_i + eo_j - ev_a - ev_b)

    def arrived(x, p):
        pltpu.make_async_remote_copy(
            src_ref=recv.at[x, p, pl.ds(0, group - 1)],
            dst_ref=recv.at[x, p, pl.ds(0, group - 1)],
            send_sem=send_sem,
            recv_sem=recv_sem.at[x, p],
            device_id={"dev": peer(1)},
            device_id_type=MESH,
        ).wait_recv()

    def add(x, lo, hi):
        for p in range(lo, hi):
            arrived(x, p)
        depth = (hi - lo) * group * SUB
        for h in range(2):
            parts = [recv[x, lo:hi, :, (2 * h + g) * SUB:(2 * h + g + 1) * SUB, :].reshape(depth, 128) for g in range(2)]
            part = dot(l4[:, lo * group * SUB:hi * group * SUB], jnp.concatenate(parts, axis=1))
            vacc[x, h] = part if lo == 0 else vacc[x, h] + part

    def energies(x):
        @pl.loop(0, o // 2, unroll=o // 2)
        def _(i):
            mats = []
            for i2 in range(2):
                at = pl.ds(pl.multiple_of((2 * i + i2) * SUB, SUB), SUB)
                mats += [vacc[x, g // 2, at, g % 2 * 128:(g % 2 + 1) * 128] for g in range(v // SUB)]
            mat = jnp.concatenate(mats, axis=0)
            mat_t = jnp.transpose(mat)
            turned = pltpu.roll(jnp.concatenate([mat_t[v:], mat_t[:v]], axis=0), v, 1)
            swap = jnp.where(first == even, mat_t, turned)
            term = mat * (2.0 * mat - swap) * rden[x, i]
            for i2 in range(2):
                esum[x, 2 * i + i2] = jnp.sum(term[i2 * v:(i2 + 1) * v].reshape(v // 8, 8, 128), axis=0)

    lane = iota((o, 128), 1)
    out = jnp.zeros((o, 128), F32)
    for x in range(2):
        add(x, 0, 8)
        add(x, 8, 12)
        add(x, 12, rows)
        energies(x)
        both = jnp.sum(esum[x], axis=1)
        for jh in range(2):
            total = jnp.sum(jnp.where(lane // v == jh, both, 0.0), axis=1, keepdims=True)
            out = jnp.where(lane == 2 * x + jh, total, out)
    e_ref[...] = jnp.transpose(out)[:o // group, :]

    pltpu.make_async_remote_copy(
        src_ref=gsend.at[:, pl.ds(0, (group - 1) * 2 * v)],
        dst_ref=gsend.at[:, pl.ds(0, (group - 1) * 2 * v)],
        send_sem=send_sem,
        recv_sem=recv_sem.at[0, 0],
        device_id={"dev": peer(1)},
        device_id_type=MESH,
    ).wait_send()


def solution(mesh):
    group = mesh.shape["dev"]

    def per_device(a_ints, c_occ, c_vir, eps_occ, eps_vir):
        rows, n = a_ints.shape[:2]
        o, v = c_occ.shape[1], c_vir.shape[1]
        hbm = pl.BlockSpec(memory_space=pltpu.HBM)
        return pl.pallas_call(
            functools.partial(kernel, n, o, v, group, rows),
            out_shape=pltpu.VMEM((o // group, o), F32),
            in_specs=[hbm] * 5,
            out_specs=pl.BlockSpec(memory_space=pltpu.VMEM),
            scratch_shapes=[
                pltpu.VMEM((3, n * n, n), BF16),
                pltpu.VMEM((o, n), BF16),
                pltpu.VMEM((v, n), BF16),
                pltpu.SMEM((o,), F32),
                pltpu.VMEM((1, v), F32),
                pltpu.VMEM((64, 2 * n), BF16),
                pltpu.VMEM((256, 128), BF16),
                pltpu.VMEM((SUB * v, SUB * n), BF16),
                pltpu.VMEM((SUB * o, SUB * n), BF16),
                pltpu.VMEM((SUB * n, 256), BF16),
                pltpu.VMEM((SUB * n, 128), BF16),
                pltpu.VMEM((rows, SUB * v, 128), BF16),
                pltpu.VMEM((2, rows, group, v, 128), BF16),
                pltpu.VMEM((2, 2, SUB * o, 256), F32),
                pltpu.VMEM((2, o // 2, 128, 128), F32),
                pltpu.VMEM((2, o, 8, 128), F32),
                pltpu.SemaphoreType.DMA((3,)),
                pltpu.SemaphoreType.DMA((8,)),
                pltpu.SemaphoreType.DMA,
                pltpu.SemaphoreType.DMA((2, rows)),
            ],
            compiler_params=pltpu.CompilerParams(
                collective_id=0, has_side_effects=True, vmem_limit_bytes=40 * 2**20),
        )(*(pltpu.with_memory_space_constraint(x, pltpu.HBM)
            for x in (a_ints.reshape(rows, n * n, n), c_occ.T, c_vir.T, eps_occ, eps_vir.reshape(1, v)))).T

    return jax.shard_map(
        per_device,
        mesh=mesh,
        in_specs=(P(("frag", "dev")), P("frag"), P("frag"), P("frag"), P("frag")),
        out_specs=P("frag", "dev"),
        check_vma=False,
    )
```

```python
import functools

import jax
import jax.numpy as jnp
from jax import lax
from jax.experimental import pallas as pl
from jax.experimental.pallas import tpu as pltpu
from jax.sharding import PartitionSpec as P


MESH = pl.DeviceIdType.MESH
SUB = 16
LATE = 5
OPPOSITE, SIDE, NEAR = (6, 7), (4, 5), (2, 3, 1)
RELAY = 3
F32 = jnp.float32
BF16 = jnp.bfloat16


def iota(shape, dim):
    return lax.broadcasted_iota(jnp.int32, shape, dim)


def ones_where(cond):
    return jnp.where(cond, 1.0, 0.0).astype(BF16)


def dot(a, b):
    return jnp.dot(a, b, preferred_element_type=F32)


def dot_t(a, b):
    return lax.dot_general(a, b, (((1,), (1,)), ((), ())), preferred_element_type=F32)


def kernel(n, o, v, group, rows, a_hbm, cot_hbm, cvt_hbm, eo_hbm, ev_hbm, e_ref,
           abuf, cot, cvt, eo, ev_ref, l1, w2, l3, l4, tp, hs, gsend, recv, relay, vacc, rden, esum,
           a_sem, in_sem, send_sem, recv_sem, relay_sem, pass_sem):
    frag, me = lax.axis_index("frag"), lax.axis_index("dev")
    slots = abuf.shape[0]
    tiles = n // 4
    cuts = [tiles * c // 26 for c in (0, 9, 17, 23, 26)]

    def load(p, slot):
        return pltpu.make_async_copy(a_hbm.at[p], abuf.at[slot], a_sem.at[slot])

    def load_first(c):
        at = pl.ds(cuts[c] * 4 * n, (cuts[c + 1] - cuts[c]) * 4 * n)
        return pltpu.make_async_copy(a_hbm.at[0, at], abuf.at[0, at], in_sem.at[4 + c])

    small = [pltpu.make_async_copy(src, dst, in_sem.at[k]) for k, (src, dst) in enumerate(
        [(cot_hbm, cot), (cvt_hbm, cvt), (eo_hbm, eo), (ev_hbm, ev_ref)])]
    for copy in small:
        copy.start()
    for c in range(4):
        load_first(c).start()

    def peer(k):
        core, x, y = lax.rem(me, 2), lax.rem(me // 2, 2), me // 4
        return 4 * lax.rem(y + k // 4, 2) + 2 * lax.rem(x + k // 2 % 2, 2) + lax.rem(core + k % 2, 2)

    barrier = pltpu.get_barrier_semaphore()
    for k in range(1, group):
        pl.semaphore_signal(barrier, inc=1, device_id={"dev": peer(k)}, device_id_type=MESH)

    @pl.when(frag == 0)
    def _():
        for k in OPPOSITE:
            pl.semaphore_signal(barrier, inc=1, device_id={"frag": 1, "dev": peer(k)}, device_id_type=MESH)

    @pl.when(frag == 1)
    def _():
        pl.semaphore_signal(barrier, inc=1, device_id={"frag": 0, "dev": me}, device_id_type=MESH)

    for copy in small:
        copy.wait()

    row = iota((64, o), 0)
    perm = ones_where(2 * (row % SUB) + row // SUB % 2 == iota((64, o), 1))
    cotp = dot(perm, cot[...]).astype(BF16)
    spread = ones_where(iota((n, 2 * n), 1) % n == iota((n, 2 * n), 0))
    same = iota((64, 2 * n), 0) // 32 == iota((64, 2 * n), 1) // n
    l1[...] = jnp.where(same, dot(cotp, spread), 0.0).astype(BF16)
    spread = ones_where(iota((256, n), 0) % 128 == iota((256, n), 1))
    same = iota((256, 2 * v), 0) // 128 == iota((256, 2 * v), 1) // v
    cvt2 = jnp.concatenate([cvt[...], cvt[...]], axis=0)
    w2[...] = jnp.where(same, dot_t(spread, cvt2), 0.0).astype(BF16)
    spread = ones_where(iota((n, SUB * n), 1) // SUB == iota((n, SUB * n), 0))
    cvrep = dot(cvt[...], spread).astype(BF16)
    for j in range(SUB):
        pick = (iota((v, SUB * n), 1) % SUB == j)
        l3[j * v:(j + 1) * v, :] = jnp.where(pick, cvrep, jnp.zeros_like(cvrep))

    def send(p, x, k):
        return pltpu.make_async_remote_copy(
            src_ref=gsend.at[p, pl.ds(pl.multiple_of((2 * peer(k) + x) * v, v), v)],
            dst_ref=recv.at[x, p, me],
            send_sem=send_sem,
            recv_sem=recv_sem.at[x, p],
            device_id={"dev": peer(k)},
            device_id_type=MESH,
        )

    def aside(k):
        return pltpu.make_async_remote_copy(
            src_ref=gsend.at[RELAY, pl.ds(pl.multiple_of((2 * peer(k) + 1) * v, v), v)],
            dst_ref=relay.at[k % 2],
            send_sem=send_sem,
            recv_sem=relay_sem.at[k % 2],
            device_id={"frag": 1, "dev": me},
            device_id_type=MESH,
        )

    def onward(k):
        return pltpu.make_async_remote_copy(
            src_ref=relay.at[k % 2],
            dst_ref=recv.at[1, RELAY, me],
            send_sem=pass_sem.at[k % 2],
            recv_sem=recv_sem.at[1, RELAY],
            device_id={"frag": 0, "dev": peer(k)},
            device_id_type=MESH,
        )

    pad = jnp.zeros((2 * n, 128 - n), BF16)

    def tile(slot, t):
        base = t * 4 * n if isinstance(t, int) else pl.multiple_of(t * 4 * n, SUB)
        left = abuf[slot, pl.ds(base, 2 * n), :]
        right = abuf[slot, pl.ds(base + 2 * n, 2 * n), :]
        out = dot(l1[...], jnp.concatenate([left, pad, right, pad], axis=1)).astype(BF16)
        for qn in range(2):
            for qk in range(2):
                to = t * 64 + (2 * qn + qk) * SUB
                to = pl.ds(to if isinstance(t, int) else pl.multiple_of(to, SUB), SUB)
                for jh in range(2):
                    at = qk * 32 + jh * SUB
                    tp[to, jh * 128:(jh + 1) * 128] = out[at:at + SUB, qn * 128:(qn + 1) * 128]

    def finish(p, chip, chips):
        at = pl.ds(pl.multiple_of(chip * 4 * v, 4 * v), chips * 4 * v)
        gsend[p, at, :] = dot(l3[at, :], hs[...]).astype(BF16)

    def hand_out(p, ks, xs):
        for x in xs:
            for k in ks:
                send(p, x, k).start()

    def keep(p):
        for x in range(2):
            recv[x, p, me] = gsend[p, pl.ds(pl.multiple_of((2 * me + x) * v, v), v), :]

    for c in range(4):
        load_first(c).wait()
        if c == 2:
            for p in range(1, slots):
                load(p, p).start()
        for t in range(cuts[c], cuts[c + 1]):
            tile(0, t)
        at = slice(cuts[c] * 64, cuts[c + 1] * 64)
        hs[at, :] = dot(tp[at, :], w2[...]).astype(BF16)
    load(slots, 0).start()
    finish(0, peer(6) // 2, 1)
    pl.semaphore_wait(barrier, group + frag)
    hand_out(0, (6, 7), (0, 1))
    finish(0, peer(4) // 2, 1)
    hand_out(0, (4, 5), (0, 1))
    finish(0, me // 4 * 2, 2)
    hand_out(0, NEAR, (0, 1))
    keep(0)

    @pl.loop(1, rows)
    def _(p):
        slot = lax.rem(p, slots)
        load(p, slot).wait()
        lax.fori_loop(0, tiles, lambda t, _: tile(slot, t), None, unroll=tiles)

        @pl.when(p + slots < rows)
        def _():
            load(p + slots, slot).start()

        hs[...] = dot(tp[...], w2[...]).astype(BF16)
        gsend[p] = dot(l3[...], hs[...]).astype(BF16)
        hand_out(p, OPPOSITE + SIDE + NEAR, (0,))

        @pl.when(p < rows - LATE)
        def _():
            detour = (p == RELAY) & (frag == 0)

            @pl.when(detour)
            def _():
                for k in OPPOSITE:
                    aside(k).start()

            @pl.when(jnp.logical_not(detour))
            def _():
                hand_out(p, OPPOSITE, (1,))

            hand_out(p, SIDE + NEAR, (1,))

        @pl.when((p == RELAY + 3) & (frag == 1))
        def _():
            for k in OPPOSITE:
                aside(k).wait_recv()
                onward(k).start()

        keep(p)

    @pl.loop(rows - LATE, rows)
    def _(p):
        hand_out(p, OPPOSITE + SIDE + NEAR, (1,))

    lane = iota((n, SUB * n), 1) // SUB
    spread = ones_where(lane % group * rows + lane // group == iota((n, SUB * n), 0))
    corep = dot(cot[...], spread).astype(BF16)
    split = ones_where(iota((SUB * o, o), 0) // SUB == iota((SUB * o, o), 1))
    diag = iota((SUB * o, SUB * n), 0) % SUB == iota((SUB * o, SUB * n), 1) % SUB
    l4[...] = jnp.where(diag, dot(split, corep), 0.0).astype(BF16)

    ev = ev_ref[...]
    ev_b = jnp.concatenate([ev, ev], axis=1)
    ev_a = jnp.transpose(jnp.broadcast_to(ev_b, (128, 128)))
    first = iota((128, 128), 0) < v
    even = iota((128, 128), 1) < v

    @pl.loop(0, o // 2)
    def _(i):
        eo_i = jnp.where(first, eo[2 * i], eo[2 * i + 1])
        for x in range(2):
            at = me * (o // group) + 2 * x
            eo_j = jnp.where(even, eo[at], eo[at + 1])
            rden[x, i] = 1.0 / (eo_i + eo_j - ev_a - ev_b)

    def arrived(x, p):
        pltpu.make_async_remote_copy(
            src_ref=recv.at[x, p, pl.ds(0, group - 1)],
            dst_ref=recv.at[x, p, pl.ds(0, group - 1)],
            send_sem=send_sem,
            recv_sem=recv_sem.at[x, p],
            device_id={"dev": peer(1)},
            device_id_type=MESH,
        ).wait_recv()

    def add(x, lo, hi):
        for p in range(lo, hi):
            arrived(x, p)
        depth = (hi - lo) * group * SUB
        for h in range(2):
            parts = [recv[x, lo:hi, :, (2 * h + g) * SUB:(2 * h + g + 1) * SUB, :].reshape(depth, 128) for g in range(2)]
            part = dot(l4[:, lo * group * SUB:hi * group * SUB], jnp.concatenate(parts, axis=1))
            vacc[x, h] = part if lo == 0 else vacc[x, h] + part

    def energies(x):
        @pl.loop(0, o // 2, unroll=o // 2)
        def _(i):
            mats = []
            for i2 in range(2):
                at = pl.ds(pl.multiple_of((2 * i + i2) * SUB, SUB), SUB)
                mats += [vacc[x, g // 2, at, g % 2 * 128:(g % 2 + 1) * 128] for g in range(v // SUB)]
            mat = jnp.concatenate(mats, axis=0)
            mat_t = jnp.transpose(mat)
            left, right = mat_t[:v], mat_t[v:]
            turned = pltpu.roll(jnp.where(even[:v], right, left), v, 1)
            swap = jnp.concatenate([jnp.where(even[:v], left, turned), jnp.where(even[:v], turned, right)], axis=0)
            term = mat * (2.0 * mat - swap) * rden[x, i]
            for i2 in range(2):
                esum[x, 2 * i + i2] = jnp.sum(term[i2 * v:(i2 + 1) * v].reshape(v // 8, 8, 128), axis=0)

    for x in range(2):
        add(x, 0, 8)
        add(x, 8, 12)
        add(x, 12, rows)
        energies(x)
        both = jnp.transpose(jnp.sum(esum[x], axis=1))
        for jh in range(2):
            e_ref[pl.ds(2 * x + jh, 1), :] = jnp.sum(both[jh * v:(jh + 1) * v], axis=0, keepdims=True)

    pltpu.make_async_remote_copy(
        src_ref=gsend.at[:, pl.ds(0, (group - 1) * 2 * v)],
        dst_ref=gsend.at[:, pl.ds(0, (group - 1) * 2 * v)],
        send_sem=send_sem,
        recv_sem=recv_sem.at[0, 0],
        device_id={"dev": peer(1)},
        device_id_type=MESH,
    ).wait_send()

    @pl.when(frag == 1)
    def _():
        for k in OPPOSITE:
            onward(k).wait_send()


def solution(mesh):
    group = mesh.shape["dev"]

    def per_device(a_ints, c_occ, c_vir, eps_occ, eps_vir):
        rows, n = a_ints.shape[:2]
        o, v = c_occ.shape[1], c_vir.shape[1]
        hbm = pl.BlockSpec(memory_space=pltpu.HBM)
        return pl.pallas_call(
            functools.partial(kernel, n, o, v, group, rows),
            out_shape=pltpu.VMEM((o // group, o), F32),
            in_specs=[hbm] * 5,
            out_specs=pl.BlockSpec(memory_space=pltpu.VMEM),
            scratch_shapes=[
                pltpu.VMEM((3, n * n, n), BF16),
                pltpu.VMEM((o, n), BF16),
                pltpu.VMEM((v, n), BF16),
                pltpu.SMEM((o,), F32),
                pltpu.VMEM((1, v), F32),
                pltpu.VMEM((64, 2 * n), BF16),
                pltpu.VMEM((256, 128), BF16),
                pltpu.VMEM((SUB * v, SUB * n), BF16),
                pltpu.VMEM((SUB * o, SUB * n), BF16),
                pltpu.VMEM((SUB * n, 256), BF16),
                pltpu.VMEM((SUB * n, 128), BF16),
                pltpu.VMEM((rows, SUB * v, 128), BF16),
                pltpu.VMEM((2, rows, group, v, 128), BF16),
                pltpu.VMEM((2, v, 128), BF16),
                pltpu.VMEM((2, 2, SUB * o, 256), F32),
                pltpu.VMEM((2, o // 2, 128, 128), F32),
                pltpu.VMEM((2, o, 8, 128), F32),
                pltpu.SemaphoreType.DMA((3,)),
                pltpu.SemaphoreType.DMA((8,)),
                pltpu.SemaphoreType.DMA,
                pltpu.SemaphoreType.DMA((2, rows)),
                pltpu.SemaphoreType.DMA((2,)),
                pltpu.SemaphoreType.DMA((2,)),
            ],
            compiler_params=pltpu.CompilerParams(
                collective_id=0, has_side_effects=True, vmem_limit_bytes=40 * 2**20),
        )(*(pltpu.with_memory_space_constraint(x, pltpu.HBM)
            for x in (a_ints.reshape(rows, n * n, n), c_occ.T, c_vir.T, eps_occ, eps_vir.reshape(1, v)))).T

    return jax.shard_map(
        per_device,
        mesh=mesh,
        in_specs=(P(("frag", "dev")), P("frag"), P("frag"), P("frag"), P("frag")),
        out_specs=P("frag", "dev"),
        check_vma=False,
    )
```

```python
import functools

import jax
import jax.numpy as jnp
from jax import lax
from jax.experimental import pallas as pl
from jax.experimental.pallas import tpu as pltpu
from jax.sharding import PartitionSpec as P


MESH = pl.DeviceIdType.MESH
SUB = 16
LATE = 5
OPPOSITE, SIDE, NEAR = (6, 7), (4, 5), (2, 3, 1)
RELAY = 3
F32 = jnp.float32
BF16 = jnp.bfloat16


def iota(shape, dim):
    return lax.broadcasted_iota(jnp.int32, shape, dim)


def ones_where(cond):
    return jnp.where(cond, 1.0, 0.0).astype(BF16)


def dot(a, b):
    return jnp.dot(a, b, preferred_element_type=F32)


def dot_t(a, b):
    return lax.dot_general(a, b, (((1,), (1,)), ((), ())), preferred_element_type=F32)


def kernel(n, o, v, group, rows, a_hbm, cot_hbm, cvt_hbm, eo_hbm, ev_hbm, e_ref,
           abuf, cot, cvt, eo, ev_ref, l1, w2, l3, l4, tp, hs, gsend, recv, relay, vacc, rden, esum,
           a_sem, in_sem, send_sem, recv_sem, relay_sem, pass_sem):
    frag, me = lax.axis_index("frag"), lax.axis_index("dev")
    slots = abuf.shape[0]
    tiles = n // 4
    cuts = [tiles * c // 26 for c in (0, 16, 26)]

    def load(p, slot):
        return pltpu.make_async_copy(a_hbm.at[p], abuf.at[slot], a_sem.at[slot])

    def load_first(c):
        at = pl.ds(cuts[c] * 4 * n, (cuts[c + 1] - cuts[c]) * 4 * n)
        return pltpu.make_async_copy(a_hbm.at[0, at], abuf.at[0, at], in_sem.at[4 + c])

    small = [pltpu.make_async_copy(src, dst, in_sem.at[k]) for k, (src, dst) in enumerate(
        [(cot_hbm, cot), (cvt_hbm, cvt), (eo_hbm, eo), (ev_hbm, ev_ref)])]
    for copy in small:
        copy.start()
    for c in range(2):
        load_first(c).start()

    def peer(k):
        core, x, y = lax.rem(me, 2), lax.rem(me // 2, 2), me // 4
        return 4 * lax.rem(y + k // 4, 2) + 2 * lax.rem(x + k // 2 % 2, 2) + lax.rem(core + k % 2, 2)

    barrier = pltpu.get_barrier_semaphore()
    for k in range(1, group):
        pl.semaphore_signal(barrier, inc=1, device_id={"dev": peer(k)}, device_id_type=MESH)

    @pl.when(frag == 0)
    def _():
        for k in OPPOSITE:
            pl.semaphore_signal(barrier, inc=1, device_id={"frag": 1, "dev": peer(k)}, device_id_type=MESH)

    @pl.when(frag == 1)
    def _():
        pl.semaphore_signal(barrier, inc=1, device_id={"frag": 0, "dev": me}, device_id_type=MESH)

    for copy in small:
        copy.wait()

    row = iota((64, o), 0)
    perm = ones_where(4 * (row % 8) + row // SUB == iota((64, o), 1))
    cotp = dot(perm, cot[...]).astype(BF16)
    spread = ones_where(iota((n, 2 * n), 1) % n == iota((n, 2 * n), 0))
    same = iota((64, 2 * n), 0) // 8 % 2 == iota((64, 2 * n), 1) // n
    l1[...] = jnp.where(same, dot(cotp, spread), 0.0).astype(BF16)
    spread = ones_where(iota((256, n), 0) % 128 == iota((256, n), 1))
    same = iota((256, 2 * v), 0) // 128 == iota((256, 2 * v), 1) // v
    cvt2 = jnp.concatenate([cvt[...], cvt[...]], axis=0)
    w2[...] = jnp.where(same, dot_t(spread, cvt2), 0.0).astype(BF16)
    depth = l3.shape[1]
    spread = ones_where(iota((n, depth), 1) // 8 == iota((n, depth), 0))
    cvrep = dot(cvt[...], spread).astype(BF16)
    for j in range(group):
        pick = iota((v, depth), 1) % 8 == j
        l3[j * v:(j + 1) * v, :] = jnp.where(pick, cvrep, jnp.zeros_like(cvrep))
    hs[8 * n:, :] = jnp.zeros((depth - 8 * n, 256), BF16)

    def send(p, x, k):
        return pltpu.make_async_remote_copy(
            src_ref=gsend.at[p, x, pl.ds(pl.multiple_of(peer(k) * v, v), v)],
            dst_ref=recv.at[x, p, me],
            send_sem=send_sem,
            recv_sem=recv_sem.at[x, p],
            device_id={"dev": peer(k)},
            device_id_type=MESH,
        )

    def aside(k):
        return pltpu.make_async_remote_copy(
            src_ref=gsend.at[RELAY, 1, pl.ds(pl.multiple_of(peer(k) * v, v), v)],
            dst_ref=relay.at[k % 2],
            send_sem=send_sem,
            recv_sem=relay_sem.at[k % 2],
            device_id={"frag": 1, "dev": me},
            device_id_type=MESH,
        )

    def onward(k):
        return pltpu.make_async_remote_copy(
            src_ref=relay.at[k % 2],
            dst_ref=recv.at[1, RELAY, me],
            send_sem=pass_sem.at[k % 2],
            recv_sem=recv_sem.at[1, RELAY],
            device_id={"frag": 0, "dev": peer(k)},
            device_id_type=MESH,
        )

    pad = jnp.zeros((2 * n, 128 - n), BF16)

    def tile(slot, t):
        base = t * 4 * n if isinstance(t, int) else pl.multiple_of(t * 4 * n, SUB)
        left = abuf[slot, pl.ds(base, 2 * n), :]
        right = abuf[slot, pl.ds(base + 2 * n, 2 * n), :]
        out = dot(l1[...], jnp.concatenate([left, pad, right, pad], axis=1)).astype(BF16)
        for qn in range(2):
            to = t * 32 + qn * SUB
            to = pl.ds(to if isinstance(t, int) else pl.multiple_of(to, SUB), SUB)
            for jq in range(4):
                tp[to, jq * 128:(jq + 1) * 128] = out[jq * SUB:(jq + 1) * SUB, qn * 128:(qn + 1) * 128]

    def second(lo, hi):
        for x in range(2):
            hs[lo:hi, x * 128:(x + 1) * 128] = dot(tp[lo:hi, x * 256:(x + 1) * 256], w2[...]).astype(BF16)

    def third(p):
        out = dot(l3[...], hs[...]).astype(BF16)
        for x in range(2):
            gsend[p, x] = out[:, x * 128:(x + 1) * 128]

    def hand_out(p, ks, xs):
        for x in xs:
            for k in ks:
                send(p, x, k).start()

    def keep(p):
        for x in range(2):
            recv[x, p, me] = gsend[p, x, pl.ds(pl.multiple_of(me * v, v), v), :]

    for c in range(2):
        load_first(c).wait()
        if c == 1:
            for p in range(1, slots):
                load(p, p).start()
        for t in range(cuts[c], cuts[c + 1]):
            tile(0, t)
        second(cuts[c] * 32, cuts[c + 1] * 32)
    load(slots, 0).start()
    third(0)
    pl.semaphore_wait(barrier, group + frag)
    hand_out(0, OPPOSITE + SIDE + NEAR, (0, 1))
    keep(0)

    @pl.loop(1, rows)
    def _(p):
        slot = lax.rem(p, slots)
        load(p, slot).wait()
        lax.fori_loop(0, tiles, lambda t, _: tile(slot, t), None, unroll=tiles)

        @pl.when(p + slots < rows)
        def _():
            load(p + slots, slot).start()

        second(0, 8 * n)
        third(p)
        hand_out(p, OPPOSITE + SIDE + NEAR, (0,))

        @pl.when(p < rows - LATE)
        def _():
            detour = (p == RELAY) & (frag == 0)

            @pl.when(detour)
            def _():
                for k in OPPOSITE:
                    aside(k).start()

            @pl.when(jnp.logical_not(detour))
            def _():
                hand_out(p, OPPOSITE, (1,))

            hand_out(p, SIDE + NEAR, (1,))

        @pl.when((p == RELAY + 3) & (frag == 1))
        def _():
            for k in OPPOSITE:
                aside(k).wait_recv()
                onward(k).start()

        keep(p)

    @pl.loop(rows - LATE, rows)
    def _(p):
        hand_out(p, OPPOSITE + SIDE + NEAR, (1,))

    lane = iota((n, SUB * n), 1) // SUB
    spread = ones_where(lane % group * rows + lane // group == iota((n, SUB * n), 0))
    corep = dot(cot[...], spread).astype(BF16)
    split = ones_where(iota((SUB * o, o), 0) // SUB == iota((SUB * o, o), 1))
    diag = iota((SUB * o, SUB * n), 0) % SUB == iota((SUB * o, SUB * n), 1) % SUB
    l4[...] = jnp.where(diag, dot(split, corep), 0.0).astype(BF16)

    ev = ev_ref[...]
    ev_b = jnp.concatenate([ev, ev], axis=1)
    ev_a = jnp.transpose(jnp.broadcast_to(ev_b, (128, 128)))
    first = iota((128, 128), 0) < v
    even = iota((128, 128), 1) < v

    @pl.loop(0, o // 2)
    def _(i):
        eo_i = jnp.where(first, eo[2 * i], eo[2 * i + 1])
        for x in range(2):
            at = me * (o // group) + 2 * x
            eo_j = jnp.where(even, eo[at], eo[at + 1])
            rden[x, i] = 1.0 / (eo_i + eo_j - ev_a - ev_b)

    def arrived(x, p):
        pltpu.make_async_remote_copy(
            src_ref=recv.at[x, p, pl.ds(0, group - 1)],
            dst_ref=recv.at[x, p, pl.ds(0, group - 1)],
            send_sem=send_sem,
            recv_sem=recv_sem.at[x, p],
            device_id={"dev": peer(1)},
            device_id_type=MESH,
        ).wait_recv()

    def add(x, lo, hi):
        for p in range(lo, hi):
            arrived(x, p)
        depth = (hi - lo) * group * SUB
        for h in range(2):
            parts = [recv[x, lo:hi, :, (2 * h + g) * SUB:(2 * h + g + 1) * SUB, :].reshape(depth, 128) for g in range(2)]
            part = dot(l4[:, lo * group * SUB:hi * group * SUB], jnp.concatenate(parts, axis=1))
            vacc[x, h] = part if lo == 0 else vacc[x, h] + part

    def energies(x):
        @pl.loop(0, o // 2, unroll=o // 2)
        def _(i):
            mats = []
            for i2 in range(2):
                at = pl.ds(pl.multiple_of((2 * i + i2) * SUB, SUB), SUB)
                mats += [vacc[x, g // 2, at, g % 2 * 128:(g % 2 + 1) * 128] for g in range(v // SUB)]
            mat = jnp.concatenate(mats, axis=0)
            mat_t = jnp.transpose(mat)
            left, right = mat_t[:v], mat_t[v:]
            turned = pltpu.roll(jnp.where(even[:v], right, left), v, 1)
            swap = jnp.concatenate([jnp.where(even[:v], left, turned), jnp.where(even[:v], turned, right)], axis=0)
            term = mat * (2.0 * mat - swap) * rden[x, i]
            for i2 in range(2):
                esum[x, 2 * i + i2] = jnp.sum(term[i2 * v:(i2 + 1) * v].reshape(v // 8, 8, 128), axis=0)

    for x in range(2):
        add(x, 0, 8)
        add(x, 8, 12)
        add(x, 12, rows)
        energies(x)
        both = jnp.transpose(jnp.sum(esum[x], axis=1))
        for jh in range(2):
            e_ref[pl.ds(2 * x + jh, 1), :] = jnp.sum(both[jh * v:(jh + 1) * v], axis=0, keepdims=True)

    pltpu.make_async_remote_copy(
        src_ref=gsend.at[:, :, pl.ds(0, (group - 1) * v)],
        dst_ref=gsend.at[:, :, pl.ds(0, (group - 1) * v)],
        send_sem=send_sem,
        recv_sem=recv_sem.at[0, 0],
        device_id={"dev": peer(1)},
        device_id_type=MESH,
    ).wait_send()

    @pl.when(frag == 1)
    def _():
        for k in OPPOSITE:
            onward(k).wait_send()


def solution(mesh):
    group = mesh.shape["dev"]

    def per_device(a_ints, c_occ, c_vir, eps_occ, eps_vir):
        rows, n = a_ints.shape[:2]
        o, v = c_occ.shape[1], c_vir.shape[1]
        hbm = pl.BlockSpec(memory_space=pltpu.HBM)
        return pl.pallas_call(
            functools.partial(kernel, n, o, v, group, rows),
            out_shape=pltpu.VMEM((o // group, o), F32),
            in_specs=[hbm] * 5,
            out_specs=pl.BlockSpec(memory_space=pltpu.VMEM),
            scratch_shapes=[
                pltpu.VMEM((3, n * n, n), BF16),
                pltpu.VMEM((o, n), BF16),
                pltpu.VMEM((v, n), BF16),
                pltpu.SMEM((o,), F32),
                pltpu.VMEM((1, v), F32),
                pltpu.VMEM((64, 2 * n), BF16),
                pltpu.VMEM((256, 128), BF16),
                pltpu.VMEM((group * v, -(-8 * n // 128) * 128), BF16),
                pltpu.VMEM((SUB * o, SUB * n), BF16),
                pltpu.VMEM((8 * n, 512), BF16),
                pltpu.VMEM((-(-8 * n // 128) * 128, 256), BF16),
                pltpu.VMEM((rows, 2, group * v, 128), BF16),
                pltpu.VMEM((2, rows, group, v, 128), BF16),
                pltpu.VMEM((2, v, 128), BF16),
                pltpu.VMEM((2, 2, SUB * o, 256), F32),
                pltpu.VMEM((2, o // 2, 128, 128), F32),
                pltpu.VMEM((2, o, 8, 128), F32),
                pltpu.SemaphoreType.DMA((3,)),
                pltpu.SemaphoreType.DMA((8,)),
                pltpu.SemaphoreType.DMA,
                pltpu.SemaphoreType.DMA((2, rows)),
                pltpu.SemaphoreType.DMA((2,)),
                pltpu.SemaphoreType.DMA((2,)),
            ],
            compiler_params=pltpu.CompilerParams(
                collective_id=0, has_side_effects=True, vmem_limit_bytes=40 * 2**20),
        )(*(pltpu.with_memory_space_constraint(x, pltpu.HBM)
            for x in (a_ints.reshape(rows, n * n, n), c_occ.T, c_vir.T, eps_occ, eps_vir.reshape(1, v)))).T

    return jax.shard_map(
        per_device,
        mesh=mesh,
        in_specs=(P(("frag", "dev")), P("frag"), P("frag"), P("frag"), P("frag")),
        out_specs=P("frag", "dev"),
        check_vma=False,
    )
```

```python
import functools

import jax
import jax.numpy as jnp
from jax import lax
from jax.experimental import pallas as pl
from jax.experimental.pallas import tpu as pltpu
from jax.sharding import PartitionSpec as P


MESH = pl.DeviceIdType.MESH
SUB = 16
LATE = 5
OPPOSITE, SIDE, NEAR = (6, 7), (4, 5), (2, 3, 1)
RELAY = 3
F32 = jnp.float32
BF16 = jnp.bfloat16


def iota(shape, dim):
    return lax.broadcasted_iota(jnp.int32, shape, dim)


def ones_where(cond):
    return jnp.where(cond, 1.0, 0.0).astype(BF16)


def dot(a, b):
    return jnp.dot(a, b, preferred_element_type=F32)


def dot_t(a, b):
    return lax.dot_general(a, b, (((1,), (1,)), ((), ())), preferred_element_type=F32)


def kernel(n, o, v, group, rows, a_hbm, cot_hbm, cvt_hbm, eo_hbm, ev_hbm, e_ref,
           abuf, cot, cvt, eo, ev_ref, l1, w2, l3, l4, tp, hs, gsend, recv, relay, vacc, rden, esum,
           a_sem, in_sem, send_sem, recv_sem, relay_sem, pass_sem):
    frag, me = lax.axis_index("frag"), lax.axis_index("dev")
    slots = abuf.shape[0]
    tiles = n // 4
    cuts = [tiles * c // 26 for c in (0, 12, 26)]

    def load(p, slot):
        return pltpu.make_async_copy(a_hbm.at[p], abuf.at[slot], a_sem.at[slot])

    def load_first(c):
        at = pl.ds(cuts[c] * 4 * n, (cuts[c + 1] - cuts[c]) * 4 * n)
        return pltpu.make_async_copy(a_hbm.at[0, at], abuf.at[0, at], in_sem.at[4 + c])

    small = [pltpu.make_async_copy(src, dst, in_sem.at[k]) for k, (src, dst) in enumerate(
        [(cot_hbm, cot), (cvt_hbm, cvt), (eo_hbm, eo), (ev_hbm, ev_ref)])]
    for copy in small:
        copy.start()
    for c in range(2):
        load_first(c).start()

    def peer(k):
        core, x, y = lax.rem(me, 2), lax.rem(me // 2, 2), me // 4
        return 4 * lax.rem(y + k // 4, 2) + 2 * lax.rem(x + k // 2 % 2, 2) + lax.rem(core + k % 2, 2)

    barrier = pltpu.get_barrier_semaphore()
    for k in range(1, group):
        pl.semaphore_signal(barrier, inc=1, device_id={"dev": peer(k)}, device_id_type=MESH)

    @pl.when(frag == 0)
    def _():
        for k in OPPOSITE:
            pl.semaphore_signal(barrier, inc=1, device_id={"frag": 1, "dev": peer(k)}, device_id_type=MESH)

    @pl.when(frag == 1)
    def _():
        pl.semaphore_signal(barrier, inc=1, device_id={"frag": 0, "dev": me}, device_id_type=MESH)

    for copy in small:
        copy.wait()

    row = iota((64, o), 0)
    perm = ones_where(4 * (row % 8) + row // SUB == iota((64, o), 1))
    cotp = dot(perm, cot[...]).astype(BF16)
    spread = ones_where(iota((n, 2 * n), 1) % n == iota((n, 2 * n), 0))
    same = iota((64, 2 * n), 0) // 8 % 2 == iota((64, 2 * n), 1) // n
    l1[...] = jnp.where(same, dot(cotp, spread), 0.0).astype(BF16)
    spread = ones_where(iota((256, n), 0) % 128 == iota((256, n), 1))
    same = iota((256, 2 * v), 0) // 128 == iota((256, 2 * v), 1) // v
    cvt2 = jnp.concatenate([cvt[...], cvt[...]], axis=0)
    w2[...] = jnp.where(same, dot_t(spread, cvt2), 0.0).astype(BF16)
    depth = l3.shape[1]
    spread = ones_where(iota((n, depth), 1) // 8 == iota((n, depth), 0))
    cvrep = dot(cvt[...], spread).astype(BF16)
    for j in range(group):
        pick = iota((v, depth), 1) % 8 == j
        l3[j * v:(j + 1) * v, :] = jnp.where(pick, cvrep, jnp.zeros_like(cvrep))
    hs[8 * n:, :] = jnp.zeros((depth - 8 * n, 256), BF16)

    def send(p, x, k):
        return pltpu.make_async_remote_copy(
            src_ref=gsend.at[p, x, pl.ds(pl.multiple_of(peer(k) * v, v), v)],
            dst_ref=recv.at[x, p, me],
            send_sem=send_sem,
            recv_sem=recv_sem.at[x, p],
            device_id={"dev": peer(k)},
            device_id_type=MESH,
        )

    def aside(k):
        return pltpu.make_async_remote_copy(
            src_ref=gsend.at[RELAY, 1, pl.ds(pl.multiple_of(peer(k) * v, v), v)],
            dst_ref=relay.at[k % 2],
            send_sem=send_sem,
            recv_sem=relay_sem.at[k % 2],
            device_id={"frag": 1, "dev": me},
            device_id_type=MESH,
        )

    def onward(k):
        return pltpu.make_async_remote_copy(
            src_ref=relay.at[k % 2],
            dst_ref=recv.at[1, RELAY, me],
            send_sem=pass_sem.at[k % 2],
            recv_sem=recv_sem.at[1, RELAY],
            device_id={"frag": 0, "dev": peer(k)},
            device_id_type=MESH,
        )

    pad = jnp.zeros((2 * n, 128 - n), BF16)

    def tile(slot, t):
        base = t * 4 * n if isinstance(t, int) else pl.multiple_of(t * 4 * n, SUB)
        left = abuf[slot, pl.ds(base, 2 * n), :]
        right = abuf[slot, pl.ds(base + 2 * n, 2 * n), :]
        out = dot(l1[...], jnp.concatenate([left, pad, right, pad], axis=1)).astype(BF16)
        for qn in range(2):
            to = t * 32 + qn * SUB
            to = pl.ds(to if isinstance(t, int) else pl.multiple_of(to, SUB), SUB)
            for jq in range(4):
                tp[to, jq * 128:(jq + 1) * 128] = out[jq * SUB:(jq + 1) * SUB, qn * 128:(qn + 1) * 128]

    def second(lo, hi):
        for x in range(2):
            hs[lo:hi, x * 128:(x + 1) * 128] = dot(tp[lo:hi, x * 256:(x + 1) * 256], w2[...]).astype(BF16)

    def third(p):
        out = dot(l3[...], hs[...]).astype(BF16)
        for x in range(2):
            gsend[p, x] = out[:, x * 128:(x + 1) * 128]

    def hand_out(p, ks, xs):
        for x in xs:
            for k in ks:
                send(p, x, k).start()

    def keep(p):
        for x in range(2):
            recv[x, p, me] = gsend[p, x, pl.ds(pl.multiple_of(me * v, v), v), :]

    for c in range(2):
        load_first(c).wait()
        if c == 1:
            for p in range(1, slots):
                load(p, p).start()
        for t in range(cuts[c], cuts[c + 1]):
            tile(0, t)
        second(cuts[c] * 32, cuts[c + 1] * 32)
    load(slots, 0).start()
    third(0)
    pl.semaphore_wait(barrier, group + frag)
    hand_out(0, OPPOSITE + SIDE + NEAR, (0, 1))
    keep(0)

    @pl.loop(1, rows)
    def _(p):
        slot = lax.rem(p, slots)
        load(p, slot).wait()
        lax.fori_loop(0, tiles, lambda t, _: tile(slot, t), None, unroll=tiles)

        @pl.when(p + slots < rows)
        def _():
            load(p + slots, slot).start()

        second(0, 8 * n)
        third(p)
        hand_out(p, OPPOSITE + SIDE + NEAR, (0,))

        @pl.when(p < rows - LATE)
        def _():
            detour = (p == RELAY) & (frag == 0)

            @pl.when(detour)
            def _():
                for k in OPPOSITE:
                    aside(k).start()

            @pl.when(jnp.logical_not(detour))
            def _():
                hand_out(p, OPPOSITE, (1,))

            hand_out(p, SIDE + NEAR, (1,))

        @pl.when((p == RELAY + 3) & (frag == 1))
        def _():
            for k in OPPOSITE:
                aside(k).wait_recv()
                onward(k).start()

        keep(p)

    @pl.loop(rows - LATE, rows)
    def _(p):
        hand_out(p, OPPOSITE, (1,))

    @pl.loop(rows - LATE, rows)
    def _(p):
        hand_out(p, SIDE + NEAR, (1,))

    lane = iota((n, SUB * n), 1) // SUB
    spread = ones_where(lane % group * rows + lane // group == iota((n, SUB * n), 0))
    corep = dot(cot[...], spread).astype(BF16)
    split = ones_where(iota((SUB * o, o), 0) // SUB == iota((SUB * o, o), 1))
    diag = iota((SUB * o, SUB * n), 0) % SUB == iota((SUB * o, SUB * n), 1) % SUB
    l4[...] = jnp.where(diag, dot(split, corep), 0.0).astype(BF16)

    ev = ev_ref[...]
    ev_b = jnp.concatenate([ev, ev], axis=1)
    ev_a = jnp.transpose(jnp.broadcast_to(ev_b, (128, 128)))
    first = iota((128, 128), 0) < v
    even = iota((128, 128), 1) < v

    @pl.loop(0, o // 2)
    def _(i):
        eo_i = jnp.where(first, eo[2 * i], eo[2 * i + 1])
        for x in range(2):
            at = me * (o // group) + 2 * x
            eo_j = jnp.where(even, eo[at], eo[at + 1])
            rden[x, i] = 1.0 / (eo_i + eo_j - ev_a - ev_b)

    def arrived(x, p):
        pltpu.make_async_remote_copy(
            src_ref=recv.at[x, p, pl.ds(0, group - 1)],
            dst_ref=recv.at[x, p, pl.ds(0, group - 1)],
            send_sem=send_sem,
            recv_sem=recv_sem.at[x, p],
            device_id={"dev": peer(1)},
            device_id_type=MESH,
        ).wait_recv()

    def add(x, lo, hi):
        for p in range(lo, hi):
            arrived(x, p)
        depth = (hi - lo) * group * SUB
        for h in range(2):
            parts = [recv[x, lo:hi, :, (2 * h + g) * SUB:(2 * h + g + 1) * SUB, :].reshape(depth, 128) for g in range(2)]
            part = dot(l4[:, lo * group * SUB:hi * group * SUB], jnp.concatenate(parts, axis=1))
            vacc[x, h] = part if lo == 0 else vacc[x, h] + part

    def energies(x):
        @pl.loop(0, o // 2, unroll=o // 2)
        def _(i):
            mats = []
            for i2 in range(2):
                at = pl.ds(pl.multiple_of((2 * i + i2) * SUB, SUB), SUB)
                mats += [vacc[x, g // 2, at, g % 2 * 128:(g % 2 + 1) * 128] for g in range(v // SUB)]
            mat = jnp.concatenate(mats, axis=0)
            mat_t = jnp.transpose(mat)
            left, right = mat_t[:v], mat_t[v:]
            turned = pltpu.roll(jnp.where(even[:v], right, left), v, 1)
            swap = jnp.concatenate([jnp.where(even[:v], left, turned), jnp.where(even[:v], turned, right)], axis=0)
            term = mat * (2.0 * mat - swap) * rden[x, i]
            for i2 in range(2):
                esum[x, 2 * i + i2] = jnp.sum(term[i2 * v:(i2 + 1) * v].reshape(v // 8, 8, 128), axis=0)

    for x in range(2):
        add(x, 0, 8)
        add(x, 8, 12)
        add(x, 12, rows)
        energies(x)
        both = jnp.transpose(jnp.sum(esum[x], axis=1))
        for jh in range(2):
            e_ref[pl.ds(2 * x + jh, 1), :] = jnp.sum(both[jh * v:(jh + 1) * v], axis=0, keepdims=True)

    pltpu.make_async_remote_copy(
        src_ref=gsend.at[:, :, pl.ds(0, (group - 1) * v)],
        dst_ref=gsend.at[:, :, pl.ds(0, (group - 1) * v)],
        send_sem=send_sem,
        recv_sem=recv_sem.at[0, 0],
        device_id={"dev": peer(1)},
        device_id_type=MESH,
    ).wait_send()

    @pl.when(frag == 1)
    def _():
        for k in OPPOSITE:
            onward(k).wait_send()


def solution(mesh):
    group = mesh.shape["dev"]

    def per_device(a_ints, c_occ, c_vir, eps_occ, eps_vir):
        rows, n = a_ints.shape[:2]
        o, v = c_occ.shape[1], c_vir.shape[1]
        hbm = pl.BlockSpec(memory_space=pltpu.HBM)
        return pl.pallas_call(
            functools.partial(kernel, n, o, v, group, rows),
            out_shape=pltpu.VMEM((o // group, o), F32),
            in_specs=[hbm] * 5,
            out_specs=pl.BlockSpec(memory_space=pltpu.VMEM),
            scratch_shapes=[
                pltpu.VMEM((3, n * n, n), BF16),
                pltpu.VMEM((o, n), BF16),
                pltpu.VMEM((v, n), BF16),
                pltpu.SMEM((o,), F32),
                pltpu.VMEM((1, v), F32),
                pltpu.VMEM((64, 2 * n), BF16),
                pltpu.VMEM((256, 128), BF16),
                pltpu.VMEM((group * v, -(-8 * n // 128) * 128), BF16),
                pltpu.VMEM((SUB * o, SUB * n), BF16),
                pltpu.VMEM((8 * n, 512), BF16),
                pltpu.VMEM((-(-8 * n // 128) * 128, 256), BF16),
                pltpu.VMEM((rows, 2, group * v, 128), BF16),
                pltpu.VMEM((2, rows, group, v, 128), BF16),
                pltpu.VMEM((2, v, 128), BF16),
                pltpu.VMEM((2, 2, SUB * o, 256), F32),
                pltpu.VMEM((2, o // 2, 128, 128), F32),
                pltpu.VMEM((2, o, 8, 128), F32),
                pltpu.SemaphoreType.DMA((3,)),
                pltpu.SemaphoreType.DMA((8,)),
                pltpu.SemaphoreType.DMA,
                pltpu.SemaphoreType.DMA((2, rows)),
                pltpu.SemaphoreType.DMA((2,)),
                pltpu.SemaphoreType.DMA((2,)),
            ],
            compiler_params=pltpu.CompilerParams(
                collective_id=0, has_side_effects=True, vmem_limit_bytes=40 * 2**20),
        )(*(pltpu.with_memory_space_constraint(x, pltpu.HBM)
            for x in (a_ints.reshape(rows, n * n, n), c_occ.T, c_vir.T, eps_occ, eps_vir.reshape(1, v)))).T

    return jax.shard_map(
        per_device,
        mesh=mesh,
        in_specs=(P(("frag", "dev")), P("frag"), P("frag"), P("frag"), P("frag")),
        out_specs=P("frag", "dev"),
        check_vma=False,
    )
```
